32 devices in a mesh: groups: 2 (over y), seq: 4 (over z), head: 2 (over x), cfg: 2 (over core).
Axes of the slice: x: 2, y: 2, z: 4, core: 2. Of those that a mesh axis runs over, the one named last changes fastest.
Arguments:
- queries: bfloat16 [2, 1024, 3072], P('cfg', ('groups', 'seq'), 'head'), parts along dimension 1, may hold values from -60 to 60
- keys: bfloat16 [2, 1024, 3072], P('cfg', ('groups', 'seq'), 'head'), parts along dimension 1, may hold values from -3 to 3
- values: bfloat16 [2, 1024, 3072], P('cfg', ('groups', 'seq'), 'head'), parts along dimension 1, may hold values from -6 to 6
- band_mask: int32 [48, 4, 4], P(('groups', 'head')), parts along dimension 0, may hold values from 0 to 1, as said below
- out_weight: bfloat16 [3072, 3072], P('head', 'cfg'), may hold values from -0.109375 to 0.109375
- guidance: float32 [1], replicated, may hold values from 3 to 8
Outputs:
- projected: bfloat16 [1024, 3072], P(('groups', 'seq'), ('cfg', 'head')), parts along dimension 0
The draws below stay inside these ranges and needn't reach their ends.
There are 2 independent parts, one for each index of `groups`. The reference program is written for one: setup_inputs(seed, part) draws one part's arguments, and reference() takes and returns one part's arrays. A program takes and returns all parts, laid end to end along the dimension named above; an argument that names none is the same for every part. Nothing has to cross between parts.
Inputs may be any that keep to these rules, and one draw needn't show every extreme that they name: `band_mask`: densities are drawn per head.
All inputs are finite; a program needn't handle non-finite values.
Results may differ from the reference program's by a relative error of at most 0.02.
Values may be sent and summed in bfloat16 or wider, within the bound.
No kernel may reach another device: no remote copies, remote signals or barrier semaphores. Data moves between devices by JAX's collectives and lax.ppermute only.
A program may use at most 128 MiB of HBM per device.

```python
import jax
import jax.numpy as jnp
from jax import lax

D = 3072
HD = 128
HEADS = 24
Q_DEV = 128
KV_DEV = 128
TILES = 4
QUERIES = 512
KEYS = 512


def shared_keys(key):
    base = jax.random.fold_in(key, 7)
    keyset = jnp.clip(jax.random.normal(base, (2, KEYS, HEADS * HD), jnp.float32), -3.0, 3.0)
    return keyset


def draw_keys(key, part):
    return shared_keys(key).astype(jnp.bfloat16)


def draw_queries(key, part):
    querset = jnp.clip(jax.random.normal(jax.random.fold_in(key, 11), (2, QUERIES, HEADS * HD), jnp.float32), -6.0, 6.0)
    return querset.astype(jnp.bfloat16)


def draw_band_mask(key, part):
    density = jax.random.randint(jax.random.fold_in(key, 21), (HEADS, 1, 1), 1, 8)
    levels = jax.random.randint(jax.random.fold_in(key, 22), (HEADS, TILES, TILES), 0, 8)
    return (levels < density).astype(jnp.int32)


def level_of(key, extent, shards, least, top_value):
    factor_of = 1.0
    for axis_at, shards_of in shards:
        heights = jax.random.uniform(jax.random.fold_in(jax.random.fold_in(key, 6), axis_at), (shards_of,), jnp.float32, least / len(shards), top_value / len(shards))
        factor_of = factor_of * jnp.repeat(jnp.exp(heights), extent[axis_at] // shards_of).reshape((-1,) + (1,) * (len(extent) - 1 - axis_at))
    return factor_of


def bell_draw(key, shape, spread, reach, cuts=(), held_as=jnp.bfloat16):
    entries = jax.random.normal(key, shape, jnp.float32) * spread
    if len(cuts) > 0:
        entries = level_of(key, shape, cuts, -0.22, 0.18) * entries
    return jnp.clip(entries, min=-reach, max=reach).astype(held_as)


def setup_inputs(seed: int = 0, part: int = 0) -> dict:
    splits = jax.random.split(jax.random.key(seed), 7)
    part_keys = jax.random.split(jax.random.fold_in(splits[6], part), 7)
    return {
        "queries": draw_queries(jax.random.fold_in(jax.random.fold_in(splits[6], part), 71), part),
        "keys": draw_keys(jax.random.fold_in(jax.random.fold_in(splits[6], part), 71), part),
        "values": bell_draw(part_keys[2], (2, KEYS, HEADS * HD), 1.0, 6.0, ((0, 2), (1, 4), (2, 2))),
        "band_mask": draw_band_mask(jax.random.fold_in(jax.random.fold_in(splits[6], part), 71), part),
        "out_weight": bell_draw(splits[4], (HEADS * HD, D), (HEADS * HD) ** -0.5, 0.109375, ((0, 2), (1, 2))),
        "guidance": jnp.clip(jax.random.uniform(splits[5], (1,), jnp.float32, 3.0, 8.0), 3.0, 8.0),
    }


def reference(queries, keys, values, band_mask, out_weight, guidance):
    scale = HD ** -0.5
    tile_of_q = (jnp.arange(QUERIES) // Q_DEV).astype(jnp.int32)
    band_of_k = (jnp.arange(KEYS) // KV_DEV).astype(jnp.int32)
    ident = jnp.eye(TILES, dtype=jnp.int32)
    qh = jnp.transpose(queries.reshape(2, QUERIES, HEADS, HD), (2, 0, 1, 3))
    kh = jnp.transpose(keys.reshape(2, KEYS, HEADS, HD), (2, 0, 1, 3))
    vh = jnp.transpose(values.reshape(2, KEYS, HEADS, HD), (2, 0, 1, 3))

    def one_head(args):
        qq, kk, vv, mask = args
        allowed = (mask + ident) > 0
        full = allowed[tile_of_q][:, band_of_k]
        outs = []
        for copy in range(2):
            scores = jnp.dot(qq[copy], kk[copy].T, preferred_element_type=jnp.float32) * scale
            scores = jnp.where(full, scores, -1e30)
            top = jnp.max(scores, axis=1, keepdims=True)
            expo = jnp.where(full, jnp.exp(scores - top), 0.0)
            total = jnp.sum(expo, axis=1, keepdims=True)
            outs.append(jnp.dot(expo.astype(jnp.bfloat16), vv[copy], preferred_element_type=jnp.float32) / total)
        return jnp.stack(outs).astype(jnp.bfloat16)

    attn = lax.map(one_head, (qh, kh, vh, band_mask))
    attn = jnp.transpose(attn, (1, 2, 0, 3)).reshape(2, QUERIES, HEADS * HD)
    cond = attn[0].astype(jnp.float32)
    uncond = attn[1].astype(jnp.float32)
    guided = (uncond + guidance[0] * (cond - uncond)).astype(jnp.bfloat16)
    return jnp.dot(guided, out_weight, preferred_element_type=jnp.float32).astype(jnp.bfloat16)
```

```python
import functools

import jax
import jax.numpy as jnp
from jax import lax
from jax.experimental import pallas as pl
from jax.experimental.pallas import tpu as pltpu
from jax.sharding import PartitionSpec as P

HD = 128
MIB = 1 << 20


def swapped(array, axis, bits):
    return lax.ppermute(array, axis, [(i, i ^ bits) for i in range(lax.axis_size(axis))])


def vmem(count):
    return [pl.BlockSpec(memory_space=pltpu.VMEM)] * count


def call(body, outs, args, flops, limit=16):
    moved = sum(a.size * a.dtype.itemsize for a in [*args, *outs])
    return pl.pallas_call(
        body,
        out_shape=outs,
        in_specs=vmem(len(args)),
        out_specs=vmem(len(outs)),
        compiler_params=pltpu.CompilerParams(vmem_limit_bytes=limit * MIB),
        cost_estimate=pl.CostEstimate(flops=flops, bytes_accessed=moved, transcendentals=0),
    )(*args)


def columns(head, count):
    return pl.ds(pl.multiple_of(head * HD, HD), count * HD)


def pack_body(slots, per, chunks, q_ref, k_ref, v_ref, *outs):
    place = lax.axis_index("seq")
    at = 0
    for first, count in chunks:
        for slot in range(slots):
            cols = columns((place ^ slot) * per + first, count)
            for part, ref in enumerate((q_ref, k_ref, v_ref)):
                outs[at][part] = ref[:, cols]
            at += 1


def attend_body(slots, first, count, scale, bias_ref, *refs):
    blocks, (keep_ref, send_ref) = refs[:slots], refs[slots:]
    rows = blocks[0].shape[1]
    half = rows // 2
    low = lax.axis_index("cfg") == 0
    for head in range(count):
        cols = slice(head * HD, (head + 1) * HD)
        keys = jnp.concatenate([b[1, :, cols] for b in blocks], axis=0)
        values = jnp.concatenate([b[2, :, cols] for b in blocks], axis=0)
        for slot in range(slots):
            scores = lax.dot_general(
                blocks[slot][0, :, cols], keys, (((1,), (1,)), ((), ())),
                preferred_element_type=jnp.float32,
            )
            line = (first + head) * slots + slot
            scores = scores * scale + bias_ref[line : line + 1, :]
            top = jnp.max(scores, axis=1, keepdims=True)
            expo = jnp.exp(scores - top)
            total = jnp.sum(expo, axis=1, keepdims=True)
            out = jnp.dot(expo.astype(jnp.bfloat16), values, preferred_element_type=jnp.float32)
            out = (out / total).astype(jnp.bfloat16)
            keep_ref[slot, :, cols] = jnp.where(low, out[:half], out[half:])
            send_ref[slot, :, cols] = jnp.where(low, out[half:], out[:half])


def guide_body(slots, scale_ref, own_ref, other_ref, *outs):
    low = lax.axis_index("cfg") == 0
    strength = scale_ref[0:1, 0:1]
    for slot in range(slots):
        own = own_ref[slot].astype(jnp.float32)
        other = other_ref[slot].astype(jnp.float32)
        cond = jnp.where(low, own, other)
        uncond = jnp.where(low, other, own)
        outs[slot][...] = (uncond + strength * (cond - uncond)).astype(jnp.bfloat16)


def join_body(slots, *refs):
    ins, out = refs[:slots], refs[slots]
    for slot in range(slots):
        out[slot] = ins[slot][...]


def project_body(slots, per, chunks, mine_side, w_ref, *refs):
    pairs, (out_ref, wide_ref) = refs[:-2], refs[-2:]
    place, core, side = lax.axis_index("seq"), lax.axis_index("cfg"), lax.axis_index("head")
    half = out_ref.shape[0] // 2
    width = out_ref.shape[1]
    for index, (first, count) in enumerate(chunks):
        mine, theirs = pairs[2 * index], pairs[2 * index + 1]
        for slot in range(slots):
            cols = columns((place ^ slot) * per + first, count)
            wide_ref[pl.ds(pl.multiple_of(core * half, half), half), cols] = mine[slot]
            wide_ref[pl.ds(pl.multiple_of((1 - core) * half, half), half), cols] = theirs[slot]
    block = side if mine_side else 1 - side
    weights = w_ref[:, pl.ds(pl.multiple_of(block * width, HD), width)]
    out_ref[...] = jnp.dot(wide_ref[...], weights, preferred_element_type=jnp.float32).astype(out_ref.dtype)


def by_heads(queries, keys, values, band_mask, out_weight, guidance):
    own_q, own_k, own_v = queries[0], keys[0], values[0]
    rows, wide = own_q.shape
    slots = lax.axis_size("seq")
    place = lax.axis_index("seq")
    per = wide // HD // slots
    chunks = [(0, per)] if per < 2 else [(0, per - per // 3), (per - per // 3, per // 3)]
    chunks = [c for c in chunks if c[1] > 0]
    half = rows // 2
    bf16, f32 = jnp.bfloat16, jnp.float32

    packed = call(
        functools.partial(pack_body, slots, per, chunks),
        [jax.ShapeDtypeStruct((3, rows, c * HD), bf16) for _, c in chunks for _ in range(slots)],
        [own_q, own_k, own_v],
        0,
    )
    order = sorted(range(1, slots), reverse=True)
    received = []
    for index in range(len(chunks)):
        got = {0: packed[index * slots]}
        for slot in order:
            got[slot] = swapped(packed[index * slots + slot], "seq", slot)
        received.append([got[s] for s in range(slots)])

    tiles = jnp.arange(slots)
    mine = lax.dynamic_slice_in_dim(band_mask, place * per, per, 0)
    pick = ((place ^ tiles)[:, None] == tiles[None, :])[None, :, None, :, None] & (
        ((place ^ tiles)[:, None] == tiles[None, :])[None, None, :, None, :]
    )
    listed = jnp.sum(jnp.where(pick, mine[:, None, None], 0), axis=(3, 4))
    allowed = (listed + jnp.eye(slots, dtype=jnp.int32)[None]) > 0
    bias = jnp.where(allowed, 0.0, -1e30).astype(f32)
    bias = jnp.repeat(bias.reshape(per * slots, slots), own_k.shape[0], axis=1)
    strength = jnp.broadcast_to(guidance.reshape(1, 1), (8, HD))

    shared = []
    for (first, count), blocks in zip(chunks, received):
        shape = jax.ShapeDtypeStruct((slots, half, count * HD), bf16)
        keep, send = call(
            functools.partial(attend_body, slots, first, count, HD ** (-0.5)),
            [shape, shape],
            [bias, *blocks],
            4 * count * (slots * rows) ** 2 * HD,
        )
        other = swapped(send, "cfg", 1)
        guided = call(
            functools.partial(guide_body, slots),
            [jax.ShapeDtypeStruct((half, count * HD), bf16)] * slots,
            [strength, keep, other],
            8 * slots * half * count * HD,
        )
        back = {0: guided[0]}
        for slot in order:
            back[slot] = swapped(guided[slot], "seq", slot)
        (mine,) = call(
            functools.partial(join_body, slots), [shape], [back[s] for s in range(slots)], 0
        )
        shared += [mine, swapped(mine, "cfg", 1)]

    width = out_weight.shape[1] // 2

    def project(mine_side, dtype):
        return pl.pallas_call(
            functools.partial(project_body, slots, per, chunks, mine_side),
            out_shape=jax.ShapeDtypeStruct((rows, width), dtype),
            in_specs=vmem(1 + len(shared)),
            out_specs=vmem(1)[0],
            scratch_shapes=[pltpu.VMEM((rows, wide), bf16)],
            compiler_params=pltpu.CompilerParams(vmem_limit_bytes=16 * MIB),
            cost_estimate=pl.CostEstimate(
                flops=2 * rows * wide * width,
                bytes_accessed=wide * width * 2,
                transcendentals=0,
            ),
        )(out_weight, *shared)

    theirs = swapped(project(False, bf16), "head", 1)
    return (project(True, f32) + theirs.astype(f32)).astype(bf16)


def by_bands(queries, keys, values, band_mask, out_weight, guidance):
    own_q = queries[0]
    own_k = keys[0]
    own_v = values[0]
    q_rows = own_q.shape[0]
    kv_rows = own_k.shape[0]
    local_heads = own_q.shape[1] // HD
    tiles = lax.axis_size("seq")
    place = lax.axis_index("seq")
    scale = HD ** (-0.5)
    bands = jnp.arange(tiles)
    ident = (bands[:, None] == bands[None, :]).astype(jnp.int32)
    allowed = band_mask + ident[None] > 0
    q_heads = own_q.reshape(q_rows, local_heads, HD)
    my_row = lax.dynamic_index_in_dim(allowed, place, 1, keepdims=False)
    k_piece = lax.all_gather(own_k, "seq", axis=0, tiled=True)
    v_piece = lax.all_gather(own_v, "seq", axis=0, tiled=True)
    count = k_piece.shape[0]
    band = jnp.arange(count) // kv_rows
    onehot = band[:, None] == bands[None, :]
    keymask = jnp.any(onehot[None] & my_row[:, None, :], axis=-1)
    k_heads = k_piece.reshape(count, local_heads, HD)
    v_heads = v_piece.reshape(count, local_heads, HD)
    scores = (
        jnp.einsum("qhd,khd->hqk", q_heads, k_heads, preferred_element_type=jnp.float32) * scale
    )
    scores = jnp.where(keymask[:, None, :], scores, -1e30)
    top = jnp.max(scores, axis=-1)
    expo = jnp.where(keymask[:, None, :], jnp.exp(scores - top[..., None]), 0.0)
    total = jnp.sum(expo, axis=-1)
    accum = jnp.einsum(
        "hqk,khd->hqd", expo.astype(jnp.bfloat16), v_heads, preferred_element_type=jnp.float32
    )
    attn = accum / total[..., None]
    own_rows = jnp.transpose(attn, (1, 0, 2)).reshape(q_rows, local_heads * HD).astype(jnp.bfloat16)
    partner = swapped(own_rows, "cfg", 1)
    first_copy = lax.axis_index("cfg") == 0
    cond = jnp.where(first_copy, own_rows, partner).astype(jnp.float32)
    uncond = jnp.where(first_copy, partner, own_rows).astype(jnp.float32)
    guided = (uncond + guidance[0] * (cond - uncond)).astype(jnp.bfloat16)
    terms = jnp.dot(guided, out_weight, preferred_element_type=jnp.float32)
    return lax.psum_scatter(terms.astype(jnp.bfloat16), "head", scatter_dimension=1, tiled=True)


def shards(queries, keys, values, band_mask, out_weight, guidance):
    slots = lax.axis_size("seq")
    heads = queries.shape[2] // HD
    rows = queries.shape[1]
    fits = heads % slots == 0 and slots & (slots - 1) == 0 and rows == keys.shape[1]
    fits = fits and rows % 32 == 0 and lax.axis_size("cfg") == 2 and lax.axis_size("head") == 2
    plan = by_heads if fits else by_bands
    return plan(queries, keys, values, band_mask, out_weight, guidance)


def solution(mesh):
    in_specs = (
        P("cfg", ("groups", "seq"), "head"),
        P("cfg", ("groups", "seq"), "head"),
        P("cfg", ("groups", "seq"), "head"),
        P(("groups", "head"), None, None),
        P("head", "cfg"),
        P(),
    )
    out_specs = P(("groups", "seq"), ("cfg", "head"))
    return jax.shard_map(shards, mesh=mesh, in_specs=in_specs, out_specs=out_specs, check_vma=False)
```

```python
import functools

import jax
import jax.numpy as jnp
from jax import lax
from jax.experimental import pallas as pl
from jax.experimental.pallas import tpu as pltpu
from jax.sharding import PartitionSpec as P


HD = 128
MIB = 1 << 20


def swapped(array, axis, bits):
    return lax.ppermute(array, axis, [(i, i ^ bits) for i in range(lax.axis_size(axis))])


def call(body, outs, args, flops, spaces=None, scratch=(), limit=16):
    moved = sum(a.size * a.dtype.itemsize for a in [*args, *outs])
    spaces = spaces or [pltpu.VMEM] * len(args)
    return pl.pallas_call(
        body,
        out_shape=outs,
        in_specs=[pl.BlockSpec(memory_space=space) for space in spaces],
        out_specs=[pl.BlockSpec(memory_space=pltpu.VMEM)] * len(outs),
        scratch_shapes=scratch,
        compiler_params=pltpu.CompilerParams(vmem_limit_bytes=limit * MIB),
        cost_estimate=pl.CostEstimate(flops=flops, bytes_accessed=moved, transcendentals=0),
    )(*args)


def columns(head, count):
    return pl.ds(pl.multiple_of(head * HD, HD), count * HD)


def start_all(copies, sem):
    copies = [pltpu.make_async_copy(src, dst, sem.at[i]) for i, (src, dst) in enumerate(copies)]
    for copy in copies:
        copy.start()
    for copy in copies:
        copy.wait()


def pack_body(slots, per, chunks, q_ref, k_ref, v_ref, *refs):
    outs, sem = refs[:-1], refs[-1]
    place = lax.axis_index("seq")
    copies = []
    for index, (first, count) in enumerate(chunks):
        for slot in range(slots):
            cols = columns((place ^ slot) * per + first, count)
            for part, ref in enumerate((q_ref, k_ref, v_ref)):
                copies.append((ref.at[:, cols], outs[index * slots + slot].at[part]))
    start_all(copies, sem)


def setup_body(slots, per, chunks, w_ref, mask_ref, guidance_ref, *refs):
    outs, (bias_ref, strength_ref, sem) = refs[:-3], refs[-3:]
    place, side = lax.axis_index("seq"), lax.axis_index("head")
    width = outs[0].shape[1]
    copies = []
    for index, (first, count) in enumerate(chunks):
        for mine in range(2):
            block = 1 - side if mine else side
            cols = pl.ds(pl.multiple_of(block * width, HD), width)
            for at in range(slots):
                src = w_ref.at[pl.ds((at * per + first) * HD, count * HD), cols]
                copies.append((src, outs[2 * index + mine].at[pl.ds(at * count * HD, count * HD)]))
    copies = [pltpu.make_async_copy(src, dst, sem.at[i]) for i, (src, dst) in enumerate(copies)]
    for copy in copies:
        copy.start()
    rows = bias_ref.shape[1] // slots
    for head in range(per):
        for slot in range(slots):
            for other in range(slots):
                listed = mask_ref[place ^ slot, place ^ other, place * per + head]
                offset = jnp.where((listed > 0) | (slot == other), 0.0, -1e30).astype(jnp.float32)
                line = head * slots + slot
                bias_ref[line : line + 1, other * rows : (other + 1) * rows] = jnp.full((1, rows), offset)
    strength_ref[...] = jnp.full(strength_ref.shape, guidance_ref[0])
    for copy in copies:
        copy.wait()


def attend_body(slots, first, count, scale, bias_ref, *refs):
    blocks, (keep_ref, send_ref) = refs[:slots], refs[slots:]
    rows = blocks[0].shape[1]
    half = rows // 2
    low = lax.axis_index("cfg") == 0
    for head in range(count):
        cols = slice(head * HD, (head + 1) * HD)
        keys = jnp.concatenate([b[1, :, cols] for b in blocks], axis=0)
        values = jnp.concatenate([b[2, :, cols] for b in blocks], axis=0)
        for slot in range(slots):
            scores = lax.dot_general(
                blocks[slot][0, :, cols], keys, (((1,), (1,)), ((), ())),
                preferred_element_type=jnp.float32,
            )
            line = (first + head) * slots + slot
            scores = scores * scale + bias_ref[line : line + 1, :]
            top = jnp.max(scores, axis=1, keepdims=True)
            expo = jnp.exp(scores - top)
            total = jnp.sum(expo, axis=1, keepdims=True)
            out = jnp.dot(expo.astype(jnp.bfloat16), values, preferred_element_type=jnp.float32)
            out = (out / total).astype(jnp.bfloat16)
            keep_ref[slot, :, cols] = jnp.where(low, out[:half], out[half:])
            send_ref[slot, :, cols] = jnp.where(low, out[half:], out[:half])


def guide_body(slots, scale_ref, own_ref, other_ref, *outs):
    low = lax.axis_index("cfg") == 0
    strength = scale_ref[0:1, 0:1]
    for slot in range(slots):
        own = own_ref[slot].astype(jnp.float32)
        other = other_ref[slot].astype(jnp.float32)
        cond = jnp.where(low, own, other)
        uncond = jnp.where(low, other, own)
        outs[slot][...] = (uncond + strength * (cond - uncond)).astype(jnp.bfloat16)


def join_body(slots, *refs):
    ins, out = refs[:slots], refs[slots]
    for slot in range(slots):
        out[slot] = ins[slot][...]


def spread(wide_ref, slots, mine_ref, theirs_ref):
    place, core = lax.axis_index("seq"), lax.axis_index("cfg")
    half = mine_ref.shape[1]
    count = mine_ref.shape[2] // HD
    for slot in range(slots):
        cols = columns((place ^ slot) * count, count)
        wide_ref[pl.ds(pl.multiple_of(core * half, half), half), cols] = mine_ref[slot]
        wide_ref[pl.ds(pl.multiple_of((1 - core) * half, half), half), cols] = theirs_ref[slot]


def project_body(slots, w_ref, mine_ref, theirs_ref, out_ref, wide_ref):
    spread(wide_ref, slots, mine_ref, theirs_ref)
    out_ref[...] = jnp.dot(
        wide_ref[...], w_ref[...], preferred_element_type=jnp.float32
    ).astype(out_ref.dtype)


def finish_body(slots, sum_ref, part_ref, w_ref, mine_ref, theirs_ref, w2_ref, mine2_ref, theirs2_ref, out_ref, wide_ref):
    total = sum_ref[...] + part_ref[...].astype(jnp.float32)
    for w, mine, theirs in ((w_ref, mine_ref, theirs_ref), (w2_ref, mine2_ref, theirs2_ref)):
        spread(wide_ref, slots, mine, theirs)
        total += jnp.dot(wide_ref[...], w[...], preferred_element_type=jnp.float32)
    out_ref[...] = total.astype(out_ref.dtype)


def by_heads(queries, keys, values, band_mask, out_weight, guidance):
    own_q, own_k, own_v = queries[0], keys[0], values[0]
    rows, wide = own_q.shape
    slots = lax.axis_size("seq")
    per = wide // HD // slots
    last = max(1, per // 3)
    chunks = [(0, per - last), (per - last, last)]
    half = rows // 2
    width = out_weight.shape[1] // 2
    bf16, f32 = jnp.bfloat16, jnp.float32
    shape = jax.ShapeDtypeStruct

    packed = call(
        functools.partial(pack_body, slots, per, chunks),
        [shape((3, rows, c * HD), bf16) for _, c in chunks for _ in range(slots)],
        [own_q, own_k, own_v],
        0,
        spaces=[pltpu.HBM] * 3,
        scratch=[pltpu.SemaphoreType.DMA((3 * slots * len(chunks),))],
        limit=53,
    )
    order = sorted(range(1, slots), reverse=True)
    received = []
    for index in range(len(chunks)):
        got = {0: packed[index * slots]}
        for slot in order:
            got[slot] = swapped(packed[index * slots + slot], "seq", slot)
        received.append([got[s] for s in range(slots)])

    *weights, bias, strength = call(
        functools.partial(setup_body, slots, per, chunks),
        [shape((slots * c * HD, width), bf16) for _, c in chunks for _ in range(2)]
        + [shape((per * slots, slots * rows), f32), shape((8, HD), f32)],
        [out_weight, jnp.transpose(band_mask, (1, 2, 0)), guidance],
        10**9,
        spaces=[pltpu.HBM, pltpu.SMEM, pltpu.SMEM],
        scratch=[pltpu.SemaphoreType.DMA((2 * slots * len(chunks),))],
    )
    keep0, send0, keep1, send1 = weights
    other1 = swapped(send1, "head", 1)

    shared = []
    for (first, count), blocks in zip(chunks, received):
        block = shape((slots, half, count * HD), bf16)
        keep, send = call(
            functools.partial(attend_body, slots, first, count, HD ** (-0.5)),
            [block, block],
            [bias, *blocks],
            4 * count * (slots * rows) ** 2 * HD,
        )
        other = swapped(send, "cfg", 1)
        guided = call(
            functools.partial(guide_body, slots),
            [shape((half, count * HD), bf16)] * slots,
            [strength, keep, other],
            8 * slots * half * count * HD,
        )
        back = {0: guided[0]}
        for slot in order:
            back[slot] = swapped(guided[slot], "seq", slot)
        (mine,) = call(
            functools.partial(join_body, slots), [block],
            [back[s] for s in range(slots)], 0,
        )
        shared.append((mine, swapped(mine, "cfg", 1)))
    (mine0, theirs0), (mine1, theirs1) = shared

    def project(weight, dtype):
        depth = weight.shape[0]
        (out,) = call(
            functools.partial(project_body, slots),
            [shape((rows, width), dtype)],
            [weight, mine0, theirs0],
            2 * rows * depth * width,
            scratch=[pltpu.VMEM((rows, depth), bf16)],
        )
        return out

    part = swapped(project(send0, bf16), "head", 1)
    total = project(keep0, f32)
    mine2 = swapped(mine1, "head", 1)
    theirs2 = swapped(mine2, "cfg", 1)
    depth = keep1.shape[0]
    (out,) = call(
        functools.partial(finish_body, slots),
        [shape((rows, width), bf16)],
        [total, part, keep1, mine1, theirs1, other1, mine2, theirs2],
        4 * rows * depth * width,
        scratch=[pltpu.VMEM((rows, depth), bf16)],
    )
    return out


def by_bands(queries, keys, values, band_mask, out_weight, guidance):
    own_q = queries[0]
    own_k = keys[0]
    own_v = values[0]
    q_rows = own_q.shape[0]
    kv_rows = own_k.shape[0]
    local_heads = own_q.shape[1] // HD
    tiles = lax.axis_size("seq")
    place = lax.axis_index("seq")
    scale = HD ** (-0.5)
    bands = jnp.arange(tiles)
    ident = (bands[:, None] == bands[None, :]).astype(jnp.int32)
    allowed = band_mask + ident[None] > 0
    q_heads = own_q.reshape(q_rows, local_heads, HD)
    my_row = lax.dynamic_index_in_dim(allowed, place, 1, keepdims=False)
    k_piece = lax.all_gather(own_k, "seq", axis=0, tiled=True)
    v_piece = lax.all_gather(own_v, "seq", axis=0, tiled=True)
    count = k_piece.shape[0]
    band = jnp.arange(count) // kv_rows
    onehot = band[:, None] == bands[None, :]
    keymask = jnp.any(onehot[None] & my_row[:, None, :], axis=-1)
    k_heads = k_piece.reshape(count, local_heads, HD)
    v_heads = v_piece.reshape(count, local_heads, HD)
    scores = (
        jnp.einsum("qhd,khd->hqk", q_heads, k_heads, preferred_element_type=jnp.float32) * scale
    )
    scores = jnp.where(keymask[:, None, :], scores, -1e30)
    top = jnp.max(scores, axis=-1)
    expo = jnp.where(keymask[:, None, :], jnp.exp(scores - top[..., None]), 0.0)
    total = jnp.sum(expo, axis=-1)
    accum = jnp.einsum(
        "hqk,khd->hqd", expo.astype(jnp.bfloat16), v_heads, preferred_element_type=jnp.float32
    )
    attn = accum / total[..., None]
    own_rows = jnp.transpose(attn, (1, 0, 2)).reshape(q_rows, local_heads * HD).astype(jnp.bfloat16)
    partner = swapped(own_rows, "cfg", 1)
    first_copy = lax.axis_index("cfg") == 0
    cond = jnp.where(first_copy, own_rows, partner).astype(jnp.float32)
    uncond = jnp.where(first_copy, partner, own_rows).astype(jnp.float32)
    guided = (uncond + guidance[0] * (cond - uncond)).astype(jnp.bfloat16)
    terms = jnp.dot(guided, out_weight, preferred_element_type=jnp.float32)
    return lax.psum_scatter(terms.astype(jnp.bfloat16), "head", scatter_dimension=1, tiled=True)


def shards(queries, keys, values, band_mask, out_weight, guidance):
    slots = lax.axis_size("seq")
    heads = queries.shape[2] // HD
    rows = queries.shape[1]
    fits = heads % slots == 0 and heads // slots > 1 and slots & (slots - 1) == 0 and rows == keys.shape[1]
    fits = fits and rows % 32 == 0 and lax.axis_size("cfg") == 2 and lax.axis_size("head") == 2
    if not fits:
        return by_bands(queries, keys, values, band_mask, out_weight, guidance)
    return by_heads(queries, keys, values, band_mask, out_weight, guidance)


def solution(mesh):
    in_specs = (
        P("cfg", ("groups", "seq"), "head"),
        P("cfg", ("groups", "seq"), "head"),
        P("cfg", ("groups", "seq"), "head"),
        P(("groups", "head"), None, None),
        P("head", "cfg"),
        P(),
    )
    out_specs = P(("groups", "seq"), ("cfg", "head"))
    return jax.shard_map(shards, mesh=mesh, in_specs=in_specs, out_specs=out_specs, check_vma=False)
```

```python
import functools

import jax
import jax.numpy as jnp
from jax import lax
from jax.experimental import pallas as pl
from jax.experimental.pallas import tpu as pltpu
from jax.sharding import PartitionSpec as P


HD = 128
MIB = 1 << 20
PACK_MIB = 52.5
FETCH_MIB = 48


def swapped(array, axis, bits):
    return lax.ppermute(array, axis, [(i, i ^ bits) for i in range(lax.axis_size(axis))])


def call(body, outs, args, flops, spaces=None, scratch=(), limit=16):
    moved = sum(a.size * a.dtype.itemsize for a in [*args, *outs])
    spaces = spaces or [pltpu.VMEM] * len(args)
    return pl.pallas_call(
        body,
        out_shape=outs,
        in_specs=[pl.BlockSpec(memory_space=space) for space in spaces],
        out_specs=[pl.BlockSpec(memory_space=pltpu.VMEM)] * len(outs),
        scratch_shapes=scratch,
        compiler_params=pltpu.CompilerParams(vmem_limit_bytes=int(limit * MIB)),
        cost_estimate=pl.CostEstimate(flops=flops, bytes_accessed=moved, transcendentals=0),
    )(*args)


def columns(head, count):
    return pl.ds(pl.multiple_of(head * HD, HD), count * HD)


def pack_body(slots, per, chunks, q_ref, k_ref, v_ref, *refs):
    outs, (held_ref, sem) = refs[:-2], refs[-2:]
    place = lax.axis_index("seq")
    copies = [
        pltpu.make_async_copy(ref, held_ref.at[part], sem.at[part])
        for part, ref in enumerate((q_ref, k_ref, v_ref))
    ]
    for copy in copies:
        copy.start()
    for part, copy in enumerate(copies):
        copy.wait()
        for index, (first, count) in enumerate(chunks):
            for slot in range(slots):
                cols = columns((place ^ slot) * per + first, count)
                outs[index * slots + slot][part] = held_ref[part, :, cols]


def bias_body(slots, per, mask_ref, guidance_ref, bias_ref, strength_ref):
    place = lax.axis_index("seq")
    rows = bias_ref.shape[1] // slots
    for head in range(per):
        for slot in range(slots):
            for other in range(slots):
                listed = mask_ref[place ^ slot, place ^ other, place * per + head]
                offset = jnp.where((listed > 0) | (slot == other), 0.0, -1e30).astype(jnp.float32)
                line = head * slots + slot
                bias_ref[line : line + 1, other * rows : (other + 1) * rows] = jnp.full((1, rows), offset)
    strength_ref[...] = jnp.full(strength_ref.shape, guidance_ref[0])


def fetch_body(slots, per, chunks, w_ref, *refs):
    outs, sem = refs[:-1], refs[-1]
    side = lax.axis_index("head")
    width = outs[0].shape[1]
    copies = []
    for index, (first, count) in enumerate(chunks):
        for mine in range(2):
            block = 1 - side if mine else side
            cols = pl.ds(pl.multiple_of(block * width, HD), width)
            for at in range(slots):
                src = w_ref.at[pl.ds((at * per + first) * HD, count * HD), cols]
                copies.append((src, outs[2 * index + mine].at[pl.ds(at * count * HD, count * HD)]))
    copies = [pltpu.make_async_copy(src, dst, sem.at[i]) for i, (src, dst) in enumerate(copies)]
    for copy in copies:
        copy.start()
    for copy in copies:
        copy.wait()


def attend_body(slots, first, count, scale, bias_ref, *refs):
    blocks, outs = refs[:slots], refs[slots:]
    rows = blocks[0].shape[1]
    half = rows // 2
    low = lax.axis_index("cfg") == 0
    for head in range(count):
        cols = slice(head * HD, (head + 1) * HD)
        keys = jnp.concatenate([b[1, :, cols] for b in blocks], axis=0)
        values = jnp.concatenate([b[2, :, cols] for b in blocks], axis=0)
        for slot in range(slots):
            scores = lax.dot_general(
                blocks[slot][0, :, cols], keys, (((1,), (1,)), ((), ())),
                preferred_element_type=jnp.float32,
            )
            line = (first + head) * slots + slot
            scores = scores * scale + bias_ref[line : line + 1, :]
            top = jnp.max(scores, axis=1, keepdims=True)
            expo = jnp.exp(scores - top)
            total = jnp.sum(expo, axis=1, keepdims=True)
            out = jnp.dot(expo.astype(jnp.bfloat16), values, preferred_element_type=jnp.float32)
            out = (out / total).astype(jnp.bfloat16)
            if len(outs) == 1:
                outs[0][slot, :, cols] = out
            else:
                outs[0][slot, :, cols] = jnp.where(low, out[:half], out[half:])
                outs[1][slot, :, cols] = jnp.where(low, out[half:], out[:half])


def guide_body(slots, scale_ref, own_ref, other_ref, *outs):
    low = lax.axis_index("cfg") == 0
    strength = scale_ref[0:1, 0:1]
    for slot in range(slots):
        own = own_ref[slot].astype(jnp.float32)
        other = other_ref[slot].astype(jnp.float32)
        cond = jnp.where(low, own, other)
        uncond = jnp.where(low, other, own)
        outs[slot][...] = (uncond + strength * (cond - uncond)).astype(jnp.bfloat16)


def join_body(slots, *refs):
    ins, out = refs[:slots], refs[slots]
    for slot in range(slots):
        out[slot] = ins[slot][...]


def early_body(slots, keep_ref, send_ref, mine_ref, theirs_ref, kept_ref, sent_ref, wide_ref):
    place, core = lax.axis_index("seq"), lax.axis_index("cfg")
    half = mine_ref.shape[1]
    count = mine_ref.shape[2] // HD
    for slot in range(slots):
        cols = columns((place ^ slot) * count, count)
        wide_ref[pl.ds(pl.multiple_of(core * half, half), half), cols] = mine_ref[slot]
        wide_ref[pl.ds(pl.multiple_of((1 - core) * half, half), half), cols] = theirs_ref[slot]
    for w_ref, out_ref in ((send_ref, sent_ref), (keep_ref, kept_ref)):
        out_ref[...] = jnp.dot(wide_ref[...], w_ref[...], preferred_element_type=jnp.float32)


def late_body(slots, w_ref, sum_ref, *refs):
    blocks, (out_ref, wide_ref) = refs[:slots], refs[slots:]
    place = lax.axis_index("seq")
    count = blocks[0].shape[1] // HD
    for slot in range(slots):
        wide_ref[:, columns((place ^ slot) * count, count)] = blocks[slot][...]
    terms = jnp.dot(wide_ref[...], w_ref[...], preferred_element_type=jnp.float32)
    out_ref[...] = (sum_ref[...] + terms).astype(out_ref.dtype)


def add_body(left_ref, right_ref, out_ref):
    out_ref[...] = (left_ref[...] + right_ref[...].astype(jnp.float32)).astype(out_ref.dtype)


def by_heads(queries, keys, values, band_mask, out_weight, guidance):
    own_q, own_k, own_v = queries[0], keys[0], values[0]
    rows, wide = own_q.shape
    slots = lax.axis_size("seq")
    per = wide // HD // slots
    last = max(1, per // 3)
    chunks = [(0, per - last), (per - last, last)]
    half = rows // 2
    width = out_weight.shape[1] // 2
    bf16, f32 = jnp.bfloat16, jnp.float32
    shape = jax.ShapeDtypeStruct

    packed = call(
        functools.partial(pack_body, slots, per, chunks),
        [shape((3, rows, c * HD), bf16) for _, c in chunks for _ in range(slots)],
        [own_q, own_k, own_v],
        0,
        spaces=[pltpu.HBM] * 3,
        scratch=[pltpu.VMEM((3, rows, wide), bf16), pltpu.SemaphoreType.DMA((3,))],
        limit=PACK_MIB,
    )
    order = partners(slots)
    received = []
    for index in range(len(chunks)):
        got = {0: packed[index * slots]}
        for slot in order:
            got[slot] = swapped(packed[index * slots + slot], "seq", slot)
        received.append([got[s] for s in range(slots)])

    bias, strength = call(
        functools.partial(bias_body, slots, per),
        [shape((per * slots, slots * rows), f32), shape((8, HD), f32)],
        [jnp.transpose(band_mask, (1, 2, 0)), guidance],
        0,
        spaces=[pltpu.SMEM, pltpu.SMEM],
    )
    keep0, send0, keep1, send1 = call(
        functools.partial(fetch_body, slots, per, chunks),
        [shape((slots * c * HD, width), bf16) for _, c in chunks for _ in range(2)],
        [out_weight],
        10**9,
        spaces=[pltpu.HBM],
        scratch=[pltpu.SemaphoreType.DMA((2 * slots * len(chunks),))],
        limit=FETCH_MIB,
    )

    backs = []
    for index, ((first, count), blocks) in enumerate(zip(chunks, received)):
        part = half if index == 0 else rows
        attended = call(
            functools.partial(attend_body, slots, first, count, HD ** (-0.5)),
            [shape((slots, part, count * HD), bf16)] * (2 - index),
            [bias, *blocks],
            4 * count * (slots * rows) ** 2 * HD,
        )
        other = swapped(attended[-1], "cfg", 1)
        guided = call(
            functools.partial(guide_body, slots),
            [shape((part, count * HD), bf16)] * slots,
            [strength, attended[0], other],
            8 * slots * part * count * HD,
        )
        back = {0: guided[0]}
        for slot in order:
            back[slot] = swapped(guided[slot], "seq", slot)
        backs.append([back[s] for s in range(slots)])

    (mine0,) = call(
        functools.partial(join_body, slots), [shape((slots, half, chunks[0][1] * HD), bf16)],
        backs[0], 0,
    )
    theirs0 = swapped(mine0, "cfg", 1)
    depth = keep0.shape[0]
    kept0, sent0 = call(
        functools.partial(early_body, slots),
        [shape((rows, width), f32)] * 2,
        [keep0, send0, mine0, theirs0],
        4 * rows * depth * width,
        scratch=[pltpu.VMEM((rows, depth), bf16)],
    )

    def late(weight, total, dtype):
        depth = weight.shape[0]
        (out,) = call(
            functools.partial(late_body, slots),
            [shape((rows, width), dtype)],
            [weight, total, *backs[1]],
            2 * rows * depth * width,
            scratch=[pltpu.VMEM((rows, depth), bf16)],
        )
        return out

    part = swapped(late(send1, sent0, bf16), "head", 1)
    (out,) = call(
        add_body, [shape((rows, width), bf16)],
        [late(keep1, kept0, f32), part], rows * width,
    )
    return out


def partners(slots):
    return [s for s in range(1, slots) if s >= slots // 2] + list(range(1, slots // 2))[::-1]


def by_bands(queries, keys, values, band_mask, out_weight, guidance):
    own_q = queries[0]
    own_k = keys[0]
    own_v = values[0]
    q_rows = own_q.shape[0]
    kv_rows = own_k.shape[0]
    local_heads = own_q.shape[1] // HD
    tiles = lax.axis_size("seq")
    place = lax.axis_index("seq")
    scale = HD ** (-0.5)
    bands = jnp.arange(tiles)
    ident = (bands[:, None] == bands[None, :]).astype(jnp.int32)
    allowed = band_mask + ident[None] > 0
    q_heads = own_q.reshape(q_rows, local_heads, HD)
    my_row = lax.dynamic_index_in_dim(allowed, place, 1, keepdims=False)
    k_piece = lax.all_gather(own_k, "seq", axis=0, tiled=True)
    v_piece = lax.all_gather(own_v, "seq", axis=0, tiled=True)
    count = k_piece.shape[0]
    band = jnp.arange(count) // kv_rows
    onehot = band[:, None] == bands[None, :]
    keymask = jnp.any(onehot[None] & my_row[:, None, :], axis=-1)
    k_heads = k_piece.reshape(count, local_heads, HD)
    v_heads = v_piece.reshape(count, local_heads, HD)
    scores = (
        jnp.einsum("qhd,khd->hqk", q_heads, k_heads, preferred_element_type=jnp.float32) * scale
    )
    scores = jnp.where(keymask[:, None, :], scores, -1e30)
    top = jnp.max(scores, axis=-1)
    expo = jnp.where(keymask[:, None, :], jnp.exp(scores - top[..., None]), 0.0)
    total = jnp.sum(expo, axis=-1)
    accum = jnp.einsum(
        "hqk,khd->hqd", expo.astype(jnp.bfloat16), v_heads, preferred_element_type=jnp.float32
    )
    attn = accum / total[..., None]
    own_rows = jnp.transpose(attn, (1, 0, 2)).reshape(q_rows, local_heads * HD).astype(jnp.bfloat16)
    partner = swapped(own_rows, "cfg", 1)
    first_copy = lax.axis_index("cfg") == 0
    cond = jnp.where(first_copy, own_rows, partner).astype(jnp.float32)
    uncond = jnp.where(first_copy, partner, own_rows).astype(jnp.float32)
    guided = (uncond + guidance[0] * (cond - uncond)).astype(jnp.bfloat16)
    terms = jnp.dot(guided, out_weight, preferred_element_type=jnp.float32)
    return lax.psum_scatter(terms.astype(jnp.bfloat16), "head", scatter_dimension=1, tiled=True)


def shards(queries, keys, values, band_mask, out_weight, guidance):
    slots = lax.axis_size("seq")
    heads = queries.shape[2] // HD
    rows = queries.shape[1]
    fits = heads % slots == 0 and heads // slots > 1 and slots & (slots - 1) == 0 and rows == keys.shape[1]
    fits = fits and rows % 32 == 0 and lax.axis_size("cfg") == 2 and lax.axis_size("head") == 2
    if not fits:
        return by_bands(queries, keys, values, band_mask, out_weight, guidance)
    return by_heads(queries, keys, values, band_mask, out_weight, guidance)


def solution(mesh):
    in_specs = (
        P("cfg", ("groups", "seq"), "head"),
        P("cfg", ("groups", "seq"), "head"),
        P("cfg", ("groups", "seq"), "head"),
        P(("groups", "head"), None, None),
        P("head", "cfg"),
        P(),
    )
    out_specs = P(("groups", "seq"), ("cfg", "head"))
    return jax.shard_map(shards, mesh=mesh, in_specs=in_specs, out_specs=out_specs, check_vma=False)
```

```python
import functools

import jax
import jax.numpy as jnp
from jax import lax
from jax.experimental import pallas as pl
from jax.experimental.pallas import tpu as pltpu
from jax.sharding import PartitionSpec as P


HD = 128
LOG2E = 1.4426950408889634
MIB = 1 << 20
LEAD_MIB = 53.5
PACK_MIB = 52.75
FETCH_MIB = 48


def swapped(array, axis, bits):
    return lax.ppermute(array, axis, [(i, i ^ bits) for i in range(lax.axis_size(axis))])


def call(body, outs, args, flops, spaces=None, scratch=(), limit=16):
    moved = sum(a.size * a.dtype.itemsize for a in [*args, *outs])
    spaces = spaces or [pltpu.VMEM] * len(args)
    return pl.pallas_call(
        body,
        out_shape=outs,
        in_specs=[pl.BlockSpec(memory_space=space) for space in spaces],
        out_specs=[pl.BlockSpec(memory_space=pltpu.VMEM)] * len(outs),
        scratch_shapes=scratch,
        compiler_params=pltpu.CompilerParams(vmem_limit_bytes=int(limit * MIB)),
        cost_estimate=pl.CostEstimate(flops=flops, bytes_accessed=moved, transcendentals=0),
    )(*args)


def columns(head, count):
    return pl.ds(pl.multiple_of(head * HD, HD), count * HD)


def lead_body(taken, per, head, q_ref, k_ref, v_ref, *refs):
    outs, sem = refs[:-1], refs[-1]
    place = lax.axis_index("seq")
    copies = []
    for at, slot in enumerate(taken):
        cols = columns((place ^ slot) * per, head)
        for part, ref in enumerate((q_ref, k_ref, v_ref)):
            copies.append((ref.at[:, cols], outs[at].at[part]))
    copies = [pltpu.make_async_copy(src, dst, sem.at[i]) for i, (src, dst) in enumerate(copies)]
    for copy in copies:
        copy.start()
    for copy in copies:
        copy.wait()


def pack_body(slots, taken, per, head, q_ref, k_ref, v_ref, *refs):
    outs, (give_ref, held_ref, sem) = refs[:-3], refs[-3:]
    place, core = lax.axis_index("seq"), lax.axis_index("cfg")
    copies = [
        pltpu.make_async_copy(ref, held_ref.at[part], sem.at[part])
        for part, ref in enumerate((q_ref, k_ref, v_ref))
    ]
    for copy in copies:
        copy.start()
    for part, copy in enumerate(copies):
        copy.wait()
        for at, slot in enumerate(taken):
            outs[at][part] = held_ref[part, :, columns((place ^ slot) * per, head)]
        for slot in range(slots):
            base = (place ^ slot) * per + head
            outs[len(taken) + slot][part] = held_ref[part, :, columns(base + core, 1)]
            give_ref[slot, part] = held_ref[part, :, columns(base + 1 - core, 1)]


def pair_body(slots, *refs):
    owns, taken_ref, outs = refs[:slots], refs[slots], refs[slots + 1 :]
    for slot in range(slots):
        outs[slot][0] = owns[slot][...]
        outs[slot][1] = taken_ref[slot]


def bias_body(slots, per, head, mask_ref, guidance_ref, bias_ref, strength_ref):
    place, core = lax.axis_index("seq"), lax.axis_index("cfg")
    rows = bias_ref.shape[1] // slots
    for index in range(head + 1):
        column = place * per + (index if index < head else head + core)
        for slot in range(slots):
            for other in range(slots):
                listed = mask_ref[place ^ slot, place ^ other, column]
                offset = jnp.where((listed > 0) | (slot == other), 0.0, -1e30).astype(jnp.float32)
                line = index * slots + slot
                bias_ref[line : line + 1, other * rows : (other + 1) * rows] = jnp.full((1, rows), offset)
    strength_ref[...] = jnp.full(strength_ref.shape, guidance_ref[0])


def fetch_body(slots, per, head, w_ref, *refs):
    outs, sem = refs[:-1], refs[-1]
    side, core = lax.axis_index("head"), lax.axis_index("cfg")
    width = outs[0].shape[1]
    copies = []
    for index, (first, count) in enumerate(((0, head), (head + core, 1), (head + 1 - core, 1))):
        for mine in range(2):
            block = 1 - side if mine else side
            cols = pl.ds(pl.multiple_of(block * width, HD), width)
            for at in range(slots):
                src = w_ref.at[columns(at * per + first, count), cols]
                copies.append((src, outs[2 * index + mine].at[pl.ds(at * count * HD, count * HD)]))
    copies = [pltpu.make_async_copy(src, dst, sem.at[i]) for i, (src, dst) in enumerate(copies)]
    for copy in copies:
        copy.start()
    for copy in copies:
        copy.wait()


def attention(scale, queries, keys, values, bias):
    scores = [
        lax.dot_general(q, k, (((1,), (1,)), ((), ())), preferred_element_type=jnp.float32)
        for q, k in zip(queries, keys)
    ]
    for head, (score, value) in enumerate(zip(scores, values)):
        lines = bias[head]
        rows = score.shape[0] // len(lines)
        for slot, line in enumerate(lines):
            tile = score[slot * rows : (slot + 1) * rows] * scale + line
            expo = jnp.exp2(tile - jnp.max(tile, axis=1, keepdims=True))
            total = jnp.sum(expo, axis=1, keepdims=True)
            out = jnp.dot(expo.astype(jnp.bfloat16), value, preferred_element_type=jnp.float32)
            yield head, slot, (out * (1.0 / total)).astype(jnp.bfloat16)


def attend_body(slots, count, scale, bias_ref, *refs):
    blocks, (keep_ref, send_ref) = refs[:slots], refs[slots:]
    half = blocks[0].shape[1] // 2
    low = lax.axis_index("cfg") == 0
    parts = [
        [
            jnp.concatenate([b[part, :, head * HD : (head + 1) * HD] for b in blocks], axis=0)
            for head in range(count)
        ]
        for part in range(3)
    ]
    bias = [[bias_ref[h * slots + s : h * slots + s + 1, :] for s in range(slots)] for h in range(count)]
    for head, slot, out in attention(scale, *parts, bias):
        cols = slice(head * HD, (head + 1) * HD)
        keep_ref[slot, :, cols] = jnp.where(low, out[:half], out[half:])
        send_ref[slot, :, cols] = jnp.where(low, out[half:], out[:half])


def attend_pair_body(slots, taken, head, scale, bias_ref, strength_ref, *refs):
    blocks, outs = refs[:slots], refs[slots:]
    low = lax.axis_index("cfg") == 0
    strength = strength_ref[0:1, 0:1]
    parts = [
        [
            jnp.concatenate([blocks[s][copy, part] for s in (range(slots) if part else taken)], axis=0)
            for copy in range(2)
        ]
        for part in range(3)
    ]
    lines = [bias_ref[head * slots + s : head * slots + s + 1, :] for s in taken]
    found = {}
    for copy, slot, out in attention(scale, *parts, [lines, lines]):
        found[copy, slot] = out.astype(jnp.float32)
        if copy == 1:
            cond = jnp.where(low, found[0, slot], found[1, slot])
            uncond = jnp.where(low, found[1, slot], found[0, slot])
            outs[slot][...] = (uncond + strength * (cond - uncond)).astype(jnp.bfloat16)


def guide_body(slots, scale_ref, own_ref, other_ref, *outs):
    low = lax.axis_index("cfg") == 0
    strength = scale_ref[0:1, 0:1]
    for slot in range(slots):
        own = own_ref[slot].astype(jnp.float32)
        other = other_ref[slot].astype(jnp.float32)
        cond = jnp.where(low, own, other)
        uncond = jnp.where(low, other, own)
        outs[slot][...] = (uncond + strength * (cond - uncond)).astype(jnp.bfloat16)


def join_body(slots, *refs):
    ins, out = refs[:-1], refs[-1]
    for slot in range(slots):
        out[slot] = ins[slot][...]


def early_body(slots, keep_ref, send_ref, mine_ref, theirs_ref, kept_ref, sent_ref, wide_ref):
    place, core = lax.axis_index("seq"), lax.axis_index("cfg")
    half = mine_ref.shape[1]
    count = mine_ref.shape[2] // HD
    for slot in range(slots):
        cols = columns((place ^ slot) * count, count)
        wide_ref[pl.ds(pl.multiple_of(core * half, half), half), cols] = mine_ref[slot]
        wide_ref[pl.ds(pl.multiple_of((1 - core) * half, half), half), cols] = theirs_ref[slot]
    for w_ref, out_ref in ((send_ref, sent_ref), (keep_ref, kept_ref)):
        out_ref[...] = jnp.dot(wide_ref[...], w_ref[...], preferred_element_type=jnp.float32)


def middle_body(slots, keep_ref, send_ref, kept_ref, sent_ref, heads_ref, kept2_ref, sent2_ref, wide_ref):
    place = lax.axis_index("seq")
    for slot in range(slots):
        wide_ref[:, columns(place ^ slot, 1)] = heads_ref[slot]
    for w_ref, sum_ref, out_ref in ((send_ref, sent_ref, sent2_ref), (keep_ref, kept_ref, kept2_ref)):
        terms = jnp.dot(wide_ref[...], w_ref[...], preferred_element_type=jnp.float32)
        out_ref[...] = sum_ref[...] + terms


def late_body(slots, w_ref, sum_ref, heads_ref, out_ref, wide_ref):
    place = lax.axis_index("seq")
    for slot in range(slots):
        wide_ref[:, columns(place ^ slot, 1)] = heads_ref[slot]
    terms = jnp.dot(wide_ref[...], w_ref[...], preferred_element_type=jnp.float32)
    out_ref[...] = (sum_ref[...] + terms).astype(out_ref.dtype)


def add_body(left_ref, right_ref, out_ref):
    out_ref[...] = (left_ref[...] + right_ref[...].astype(jnp.float32)).astype(out_ref.dtype)


def by_heads(queries, keys, values, band_mask, out_weight, guidance):
    own_q, own_k, own_v = queries[0], keys[0], values[0]
    rows, wide = own_q.shape
    slots = lax.axis_size("seq")
    per = wide // HD // slots
    head = per - 2
    half = rows // 2
    width = out_weight.shape[1] // 2
    bf16, f32 = jnp.bfloat16, jnp.float32
    shape = jax.ShapeDtypeStruct
    order = partners(slots)
    far, near = [s for s in order if s >= slots // 2], [s for s in order if s < slots // 2]
    scale = HD ** (-0.5) * LOG2E

    rest = near + [0]
    lead = shape((3, rows, head * HD), bf16)
    sources = [own_q, own_k, own_v]
    led = call(
        functools.partial(lead_body, far, per, head),
        [lead] * len(far),
        sources,
        0,
        spaces=[pltpu.HBM] * 3,
        scratch=[pltpu.SemaphoreType.DMA((3 * len(far),))],
        limit=LEAD_MIB,
    )
    *packed, give = call(
        functools.partial(pack_body, slots, rest, per, head),
        [lead] * len(rest) + [shape((3, rows, HD), bf16)] * slots + [shape((slots, 3, rows, HD), bf16)],
        sources,
        0,
        spaces=[pltpu.HBM] * 3,
        scratch=[pltpu.VMEM((3, rows, wide), bf16), pltpu.SemaphoreType.DMA((3,))],
        limit=PACK_MIB,
    )
    led = dict(zip(far + rest, [*led, *packed]))
    blocks0 = {s: swapped(led[s], "seq", s) for s in order} | {0: led[0]}
    taken = swapped(give, "cfg", 1)
    paired = call(
        functools.partial(pair_body, slots),
        [shape((2, 3, rows, HD), bf16)] * slots,
        [*packed[len(rest) :], taken],
        0,
    )
    blocks1 = {s: swapped(paired[s], "seq", s) for s in order} | {0: paired[0]}

    bias, strength = call(
        functools.partial(bias_body, slots, per, head),
        [shape(((head + 1) * slots, slots * rows), f32), shape((8, HD), f32)],
        [jnp.transpose(band_mask, (1, 2, 0)), guidance],
        0,
        spaces=[pltpu.SMEM, pltpu.SMEM],
    )
    keep0, send0, keep1, send1, keep2, send2 = call(
        functools.partial(fetch_body, slots, per, head),
        [shape((slots * c * HD, width), bf16) for c in (head, 1, 1) for _ in range(2)],
        [out_weight],
        10**9,
        spaces=[pltpu.HBM],
        scratch=[pltpu.SemaphoreType.DMA((6 * slots,))],
        limit=FETCH_MIB,
    )

    keep, send = call(
        functools.partial(attend_body, slots, head, scale),
        [shape((slots, half, head * HD), bf16)] * 2,
        [bias, *(blocks0[s] for s in range(slots))],
        4 * head * (slots * rows) ** 2 * HD,
    )
    other = swapped(send, "cfg", 1)
    guided0 = call(
        functools.partial(guide_body, slots),
        [shape((half, head * HD), bf16)] * slots,
        [strength, keep, other],
        8 * slots * half * head * HD,
    )
    guided1 = {}
    for taken in (far + near + [0],):
        found = call(
            functools.partial(attend_pair_body, slots, taken, head, scale),
            [shape((rows, HD), bf16)] * len(taken),
            [bias, strength, *(blocks1[s] for s in range(slots))],
            8 * len(taken) * slots * rows**2 * HD,
        )
        guided1 |= dict(zip(taken, found))
    shared = []
    for guided in (guided0, guided1):
        back = {s: swapped(guided[s], "seq", s) for s in order} | {0: guided[0]}
        back = [back[s] for s in range(slots)]
        (mine,) = call(
            functools.partial(join_body, slots), [shape((slots, *guided[0].shape), bf16)], back, 0
        )
        shared += [mine, swapped(mine, "cfg", 1)]
    mine0, theirs0, mine1, theirs1 = shared

    def project(body, outs, args):
        depth = args[0].shape[0]
        return call(
            functools.partial(body, slots),
            outs,
            args,
            2 * len(outs) * rows * depth * width,
            scratch=[pltpu.VMEM((rows, depth), bf16)],
        )

    sums = [shape((rows, width), f32)] * 2
    kept, sent = project(early_body, sums, [keep0, send0, mine0, theirs0])
    kept, sent = project(middle_body, sums, [keep1, send1, kept, sent, mine1])
    (sent,) = project(late_body, [shape((rows, width), bf16)], [send2, sent, theirs1])
    part = swapped(sent, "head", 1)
    (kept,) = project(late_body, sums[:1], [keep2, kept, theirs1])
    (out,) = call(add_body, [shape((rows, width), bf16)], [kept, part], rows * width)
    return out


def partners(slots):
    return [s for s in range(1, slots) if s >= slots // 2] + list(range(1, slots // 2))[::-1]


def by_bands(queries, keys, values, band_mask, out_weight, guidance):
    own_q = queries[0]
    own_k = keys[0]
    own_v = values[0]
    q_rows = own_q.shape[0]
    kv_rows = own_k.shape[0]
    local_heads = own_q.shape[1] // HD
    tiles = lax.axis_size("seq")
    place = lax.axis_index("seq")
    scale = HD ** (-0.5)
    bands = jnp.arange(tiles)
    ident = (bands[:, None] == bands[None, :]).astype(jnp.int32)
    allowed = band_mask + ident[None] > 0
    q_heads = own_q.reshape(q_rows, local_heads, HD)
    my_row = lax.dynamic_index_in_dim(allowed, place, 1, keepdims=False)
    k_piece = lax.all_gather(own_k, "seq", axis=0, tiled=True)
    v_piece = lax.all_gather(own_v, "seq", axis=0, tiled=True)
    count = k_piece.shape[0]
    band = jnp.arange(count) // kv_rows
    onehot = band[:, None] == bands[None, :]
    keymask = jnp.any(onehot[None] & my_row[:, None, :], axis=-1)
    k_heads = k_piece.reshape(count, local_heads, HD)
    v_heads = v_piece.reshape(count, local_heads, HD)
    scores = (
        jnp.einsum("qhd,khd->hqk", q_heads, k_heads, preferred_element_type=jnp.float32) * scale
    )
    scores = jnp.where(keymask[:, None, :], scores, -1e30)
    top = jnp.max(scores, axis=-1)
    expo = jnp.where(keymask[:, None, :], jnp.exp(scores - top[..., None]), 0.0)
    total = jnp.sum(expo, axis=-1)
    accum = jnp.einsum(
        "hqk,khd->hqd", expo.astype(jnp.bfloat16), v_heads, preferred_element_type=jnp.float32
    )
    attn = accum / total[..., None]
    own_rows = jnp.transpose(attn, (1, 0, 2)).reshape(q_rows, local_heads * HD).astype(jnp.bfloat16)
    partner = swapped(own_rows, "cfg", 1)
    first_copy = lax.axis_index("cfg") == 0
    cond = jnp.where(first_copy, own_rows, partner).astype(jnp.float32)
    uncond = jnp.where(first_copy, partner, own_rows).astype(jnp.float32)
    guided = (uncond + guidance[0] * (cond - uncond)).astype(jnp.bfloat16)
    terms = jnp.dot(guided, out_weight, preferred_element_type=jnp.float32)
    return lax.psum_scatter(terms.astype(jnp.bfloat16), "head", scatter_dimension=1, tiled=True)


def shards(queries, keys, values, band_mask, out_weight, guidance):
    slots = lax.axis_size("seq")
    heads = queries.shape[2] // HD
    rows = queries.shape[1]
    fits = heads % slots == 0 and heads // slots > 2 and slots & (slots - 1) == 0 and rows == keys.shape[1]
    fits = fits and rows % 32 == 0 and lax.axis_size("cfg") == 2 and lax.axis_size("head") == 2
    if not fits:
        return by_bands(queries, keys, values, band_mask, out_weight, guidance)
    return by_heads(queries, keys, values, band_mask, out_weight, guidance)


def solution(mesh):
    in_specs = (
        P("cfg", ("groups", "seq"), "head"),
        P("cfg", ("groups", "seq"), "head"),
        P("cfg", ("groups", "seq"), "head"),
        P(("groups", "head"), None, None),
        P("head", "cfg"),
        P(),
    )
    out_specs = P(("groups", "seq"), ("cfg", "head"))
    return jax.shard_map(shards, mesh=mesh, in_specs=in_specs, out_specs=out_specs, check_vma=False)
```
